32 devices in a mesh: tm: 16 (over z, y, core), user: 2 (over x).
Axes of the slice: x: 2, y: 2, z: 4, core: 2. Of those that a mesh axis runs over, the one named last changes fastest.
Arguments:
- events: bfloat16 [64, 1024, 256], P('user', 'tm'), parts along dimension 0, may hold values from -6 to 6
- lengths: int32 [64], P('user'), parts along dimension 0, may hold values from 256 to 1024
- w_mix: bfloat16 [2, 256, 256], replicated, may hold values from -0.375 to 0.375
- w_context: bfloat16 [2, 256, 256], replicated, may hold values from -0.375 to 0.375
- gains: float32 [2, 256], replicated, may hold values from 0.5 to 1.5
- w_up: bfloat16 [2, 256, 1024], replicated, may hold values from -0.375 to 0.375
- w_down: bfloat16 [2, 1024, 256], replicated, may hold values from -0.1875 to 0.1875
Outputs:
- encoded: bfloat16 [64, 1024, 256], P('user', 'tm'), parts along dimension 0
The draws below stay inside these ranges and needn't reach their ends.
There are 2 independent parts, one for each index of `user`. The reference program is written for one: setup_inputs(seed, part) draws one part's arguments, and reference() takes and returns one part's arrays. A program takes and returns all parts, laid end to end along the dimension named above; an argument that names none is the same for every part. Nothing has to cross between parts.
All inputs are finite; a program needn't handle non-finite values.
Results may differ from the reference program's by a relative error of at most 0.012.
Values may be sent and summed in bfloat16 or wider, within the bound.
A program may use at most 64 MiB of HBM per device.

```python
import jax
import jax.numpy as jnp
from jax import lax

D = 256
FF = 1024
HALF = 32
LAYERS = 2
USERS = 32
NT = 1024


def set_ends(values, stream_key, least, high):
    index_at = [jax.random.randint(jax.random.fold_in(stream_key, axis), (), 0, length) for axis, length in enumerate(values.shape)]
    longest = values.shape.index(max(values.shape))
    beside = index_at[:longest] + [(index_at[longest] + 1) % values.shape[longest]] + index_at[longest + 1:]
    return values.at[tuple(index_at)].set(least).at[tuple(beside)].set(high)


def level_of(stream_key, dims, cuts, smallest, high):
    def one(dim, shards_of):
        heights = jax.random.uniform(jax.random.fold_in(jax.random.fold_in(stream_key, 6), dim), (shards_of,), jnp.float32, smallest / len(cuts), high / len(cuts))
        return jnp.repeat(jnp.exp(heights), dims[dim] // shards_of).reshape((-1,) + (1,) * (len(dims) - dim - 1))

    level = one(*cuts[0])
    for cut in cuts[1:]:
        level = level * one(*cut)
    return level


def gaussian(own_key, dims, spread, limit, split=(), kind=jnp.bfloat16):
    level = level_of(own_key, dims, split, -0.22, 0.18) if split else 1.0
    values = jax.random.normal(own_key, dims, jnp.float32) * spread * level
    return jnp.minimum(jnp.maximum(values, -limit), limit).astype(kind)


def setup_inputs(seed: int = 0, part: int = 0) -> dict:
    streams_of = jax.random.split(jax.random.key(seed), 8)
    part_keys = jax.random.split(jax.random.fold_in(streams_of[7], part), 8)
    events = gaussian(part_keys[0], (USERS, NT, D), 1.0, 6.0, ((1, 16),))
    lengths = set_ends(jax.random.randint(part_keys[1], (USERS,), NT // 4, NT + 1), jax.random.fold_in(part_keys[1], 1), NT // 4, NT).astype(jnp.int32)
    w_mix = gaussian(streams_of[2], (LAYERS, D, D), D ** -0.5, 0.375)
    w_context = gaussian(streams_of[3], (LAYERS, D, D), D ** -0.5, 0.375)
    gains = jnp.clip(1.0 + 0.1 * jax.random.normal(streams_of[4], (LAYERS, D), jnp.float32), 0.5, 1.5)
    w_up = gaussian(streams_of[5], (LAYERS, D, FF), D ** -0.5, 0.375)
    w_down = gaussian(streams_of[6], (LAYERS, FF, D), FF ** -0.5, 0.1875)
    return {"events": events, "lengths": lengths, "w_mix": w_mix, "w_context": w_context, "gains": gains, "w_up": w_up, "w_down": w_down}


def apply_layer(layer_index, current, valid_mask, w_mix, w_context, gains, w_up, w_down):
    as_float = current.astype(jnp.float32)
    seq_len = current.shape[1]
    padded = jnp.pad(as_float, ((0, 0), (HALF, HALF), (0, 0)))
    mixed_rows = jnp.zeros_like(as_float)
    for offset in range(2 * HALF + 1):
        shifted = padded[:, offset:offset + seq_len]
        weight = lax.optimization_barrier(jnp.sum(as_float * shifted, axis=-1)) / D
        weight = lax.optimization_barrier(weight.astype(jnp.bfloat16)).astype(jnp.float32)
        mixed_rows = mixed_rows + weight[..., None] * shifted
    mixed_rows = mixed_rows.astype(jnp.bfloat16)
    position = jnp.arange(seq_len, dtype=jnp.int32).astype(jnp.float32)
    context = (jnp.cumsum(as_float, axis=1) / jnp.sqrt(position + 1.0)[None, :, None]).astype(jnp.bfloat16)
    flat_mix = mixed_rows.reshape(-1, D)
    flat_ctx = context.reshape(-1, D)
    compressed = jnp.dot(flat_mix, w_mix[layer_index], preferred_element_type=jnp.float32)
    compressed = compressed + jnp.dot(flat_ctx, w_context[layer_index], preferred_element_type=jnp.float32)
    summed = as_float.reshape(-1, D) + compressed
    row_mean = lax.optimization_barrier(jnp.mean(summed, axis=-1, keepdims=True))
    row_var = lax.optimization_barrier(jnp.mean((summed - row_mean) ** 2, axis=-1, keepdims=True))
    normed = ((summed - row_mean) / jnp.sqrt(row_var + 1e-05) * gains[layer_index]).astype(jnp.bfloat16)
    hidden = jax.nn.relu(jnp.dot(normed, w_up[layer_index], preferred_element_type=jnp.float32)).astype(jnp.bfloat16)
    result = normed.astype(jnp.float32) + jnp.dot(hidden, w_down[layer_index], preferred_element_type=jnp.float32)
    result = result.reshape(current.shape)
    return jnp.where(valid_mask[..., None], result, 0.0).astype(jnp.bfloat16)

def reference(events, lengths, w_mix, w_context, gains, w_up, w_down):
    position = jnp.arange(events.shape[1], dtype=jnp.int32)
    valid_mask = position[None, :] < lengths[:, None]
    current = jnp.where(valid_mask[..., None], events, jnp.zeros_like(events)).astype(jnp.bfloat16)
    for layer_index in range(LAYERS):
        current = apply_layer(layer_index, current, valid_mask, w_mix, w_context, gains, w_up, w_down)
    return current
```

```python
import functools

import jax
import jax.numpy as jnp
from jax import lax
from jax.experimental import pallas as pl
from jax.experimental.pallas import tpu as pltpu
from jax.sharding import PartitionSpec as P

HALF = 32
ROWS = 256
BLOCK = 8
EPS = 1e-05
MESH = pl.DeviceIdType.MESH


def group_size(count):
    size = 1
    while size * size < count:
        size *= 2
    return size if count % size == 0 else 1


def dot(a, b):
    return jnp.dot(a, b, preferred_element_type=jnp.float32)


def dot_t(a, b):
    return lax.dot_general(a, b, (((1,), (1,)), ((), ())), preferred_element_type=jnp.float32)


def kernel(
    count,
    lengths,
    gains,
    events,
    w_mix,
    w_context,
    w_up,
    w_down,
    out,
    x,
    result,
    low,
    high,
    mixed_own,
    mix_v,
    ctx_v,
    up_v,
    down_v,
    own_mask,
    halo_mask,
    lower_ones,
    row_scale,
    user_ones,
    totals,
    group_got,
    plane,
    cross_got,
    earlier,
    event_sem,
    weight_sem,
    out_sem,
    halo_send,
    halo_recv,
    group_send,
    group_recv,
    cross_send,
    cross_recv,
):
    layers, users, rows, width = x.shape
    steps = users // BLOCK
    per_dot = ROWS // rows
    me = lax.axis_index("tm")
    first_pos = me * rows
    group = group_got.shape[1] + 1
    groups = count // group
    in_group = lax.rem(me, group)
    my_group = lax.div(me, group)

    def event_copy(step):
        part = pl.ds(step * BLOCK, BLOCK)
        return pltpu.make_async_copy(events.at[part], x.at[0, part], event_sem.at[step])

    weight_copies = [
        pltpu.make_async_copy(source, target, weight_sem.at[i])
        for i, (source, target) in enumerate(
            ((w_mix, mix_v), (w_context, ctx_v), (w_up, up_v), (w_down, down_v))
        )
    ]
    for step in range(steps):
        event_copy(step).start()
    for copy in weight_copies:
        copy.start()

    barrier = pltpu.get_barrier_semaphore()

    def group_peer(k):
        return my_group * group + lax.rem(in_group + k, group)

    def cross_peer(k):
        return me + k * group

    for k in range(1, group):
        pl.semaphore_signal(barrier, inc=1, device_id={"tm": group_peer(k)}, device_id_type=MESH)
    for k in range(1, groups):
        other = lax.rem(me + k * group, count)
        pl.semaphore_signal(barrier, inc=1, device_id={"tm": other}, device_id_type=MESH)

    @pl.when(me > 0)
    def _():
        pl.semaphore_signal(barrier, inc=1, device_id={"tm": me - 1}, device_id_type=MESH)

    @pl.when(me < count - 1)
    def _():
        pl.semaphore_signal(barrier, inc=1, device_id={"tm": me + 1}, device_id_type=MESH)

    sides = (me > 0).astype(jnp.int32) + (me < count - 1).astype(jnp.int32)
    pl.semaphore_wait(barrier, group + groups - 2 + sides)

    def to_next(layer, step):
        part = pl.ds(step * BLOCK, BLOCK)
        source = events.at[part] if layer == 0 else x.at[layer, part]
        return pltpu.make_async_remote_copy(
            src_ref=source.at[:, pl.ds(rows - HALF, HALF)],
            dst_ref=low.at[layer, part],
            send_sem=halo_send.at[layer, 0, step],
            recv_sem=halo_recv.at[layer, 0, step],
            device_id={"tm": me + 1},
            device_id_type=MESH,
        )

    def to_previous(layer, step):
        part = pl.ds(step * BLOCK, BLOCK)
        source = events.at[part] if layer == 0 else x.at[layer, part]
        return pltpu.make_async_remote_copy(
            src_ref=source.at[:, pl.ds(0, HALF)],
            dst_ref=high.at[layer, part],
            send_sem=halo_send.at[layer, 1, step],
            recv_sem=halo_recv.at[layer, 1, step],
            device_id={"tm": me - 1},
            device_id_type=MESH,
        )

    def send_halos(layer, step):
        @pl.when(me < count - 1)
        def _():
            to_next(layer, step).start()

        @pl.when(me > 0)
        def _():
            to_previous(layer, step).start()

    def wait_halos(layer, step):
        @pl.when(me > 0)
        def _():
            to_next(layer, step).wait_recv()

        @pl.when(me < count - 1)
        def _():
            to_previous(layer, step).wait_recv()

    def wait_halo_sends(layer, step):
        @pl.when(me < count - 1)
        def _():
            to_next(layer, step).wait_send()

        @pl.when(me > 0)
        def _():
            to_previous(layer, step).wait_send()

    for step in range(steps):
        send_halos(0, step)

    row_bits, half_bits = rows.bit_length() - 1, HALF.bit_length() - 1
    target = lax.broadcasted_iota(jnp.int32, (ROWS, ROWS), 0)
    source = lax.broadcasted_iota(jnp.int32, (ROWS, ROWS), 1)
    target_user, source_user = target >> row_bits, source >> row_bits
    t, s = target & (rows - 1), source & (rows - 1)
    same = target_user == source_user
    near = (s - t <= HALF) & (t - s <= HALF)
    own_mask[...] = jnp.where(same & near, 1.0 / width, 0.0)
    lower_ones[...] = jnp.where(same & (s <= t), 1.0, 0.0).astype(jnp.bfloat16)
    side_rows = per_dot * HALF
    wide = 2 * side_rows
    target = lax.broadcasted_iota(jnp.int32, (ROWS, wide), 0)
    source = lax.broadcasted_iota(jnp.int32, (ROWS, wide), 1)
    is_high = source >= side_rows
    source = jnp.where(is_high, source - side_rows, source)
    s = (source & (HALF - 1)) + jnp.where(is_high, rows, -HALF)
    t = target & (rows - 1)
    same = (target >> row_bits) == (source >> half_bits)
    near = (s - t <= HALF) & (t - s <= HALF)
    halo_mask[...] = jnp.where(same & near, 1.0 / width, 0.0)
    position = first_pos + lax.broadcasted_iota(jnp.int32, (rows, width), 0)
    row_scale[...] = 1.0 / jnp.sqrt(position.astype(jnp.float32) + 1.0)
    user = lax.broadcasted_iota(jnp.int32, (BLOCK, BLOCK * rows), 0)
    row = lax.broadcasted_iota(jnp.int32, (BLOCK, BLOCK * rows), 1)
    user_ones[...] = jnp.where(user == (row >> row_bits), 1.0, 0.0).astype(jnp.bfloat16)

    @pl.when(me == 0)
    def _():
        low[...] = jnp.zeros_like(low)

    @pl.when(me == count - 1)
    def _():
        high[...] = jnp.zeros_like(high)

    def masked(block, step, start):
        offset = lax.broadcasted_iota(jnp.int32, block.shape[1:], 0) + start
        parts = [
            jnp.where(offset < lengths[step * BLOCK + u], block[u].astype(jnp.float32), 0.0)
            for u in range(BLOCK)
        ]
        return jnp.stack(parts).astype(jnp.bfloat16)

    def add_totals(layer, step, block):
        part = pl.ds(pl.multiple_of(step * BLOCK, BLOCK), BLOCK)
        totals[layer, part, :] = dot(user_ones[...], block.reshape(BLOCK * rows, width))

    def mask_step(step, carry):
        event_copy(step).wait()
        part = pl.ds(step * BLOCK, BLOCK)
        block = masked(x[0, part], step, first_pos)
        x[0, part] = block
        add_totals(0, step, block)
        return carry

    lax.fori_loop(0, steps, mask_step, 0)

    def group_copy(layer, k):
        return pltpu.make_async_remote_copy(
            src_ref=totals.at[layer],
            dst_ref=group_got.at[layer, k - 1],
            send_sem=group_send.at[layer, k - 1],
            recv_sem=group_recv.at[layer, k - 1],
            device_id={"tm": group_peer(k)},
            device_id_type=MESH,
        )

    def cross_copy(layer, k):
        return pltpu.make_async_remote_copy(
            src_ref=plane.at[layer],
            dst_ref=cross_got.at[layer, k - 1],
            send_sem=cross_send.at[layer, k - 1],
            recv_sem=cross_recv.at[layer, k - 1],
            device_id={"tm": cross_peer(k)},
            device_id_type=MESH,
        )

    def start_group(layer):
        for k in range(1, group):
            group_copy(layer, k).start()

    def finish_group_start_cross(layer):
        before = jnp.zeros((users, width), jnp.float32)
        whole = totals[layer]
        for k in range(1, group):
            group_copy(layer, k).wait_recv()
            got = group_got[layer, k - 1]
            whole = whole + got
            before = before + jnp.where(in_group >= k, got, 0.0)
        plane[layer] = whole
        earlier[layer] = before
        for k in range(1, groups):

            @pl.when(my_group + k < groups)
            def _(k=k):
                cross_copy(layer, k).start()

    def finish_cross(layer):
        for k in range(1, groups):

            @pl.when(my_group >= k)
            def _(k=k):
                cross_copy(layer, k).wait_recv()
                earlier[layer] += cross_got[layer, k - 1]

    def wait_sum_sends(layer):
        for k in range(1, group):
            group_copy(layer, k).wait_send()
        for k in range(1, groups):

            @pl.when(my_group + k < groups)
            def _(k=k):
                cross_copy(layer, k).wait_send()

    def own_step(layer, step, carry):
        for piece in range(BLOCK // per_dot):
            part = pl.ds(step * BLOCK + piece * per_dot, per_dot)
            block = x[layer, part].reshape(ROWS, width)
            weights = (dot_t(block, block) * own_mask[...]).astype(jnp.bfloat16)
            mixed_own[part] = dot(weights, block).reshape(per_dot, rows, width)
        return carry

    def layer_step(layer, step, carry):
        part = pl.ds(step * BLOCK, BLOCK)
        wait_halos(layer, step)
        block = x[layer, part]
        low_rows, high_rows = low[layer, part], high[layer, part]
        if layer == 0:
            low_rows = masked(low_rows, step, first_pos - HALF)
            high_rows = masked(high_rows, step, first_pos + rows)
        mixed, running = [], []
        for piece in range(BLOCK // per_dot):
            cut = slice(piece * per_dot, (piece + 1) * per_dot)
            here = block[cut].reshape(ROWS, width)
            halo = jnp.concatenate(
                [low_rows[cut].reshape(side_rows, width), high_rows[cut].reshape(side_rows, width)],
                axis=0,
            )
            weights = (dot_t(here, halo) * halo_mask[...]).astype(jnp.bfloat16)
            mixed.append(dot(weights, halo))
            running.append(dot(lower_ones[...], here))
        mixed = jnp.concatenate(mixed, axis=0) + mixed_own[part].reshape(BLOCK * rows, width)
        running = jnp.concatenate(running, axis=0).reshape(BLOCK, rows, width)
        before = earlier[layer, pl.ds(pl.multiple_of(step * BLOCK, BLOCK), BLOCK), :]
        context = (running + before[:, None, :]) * row_scale[...][None]
        context = context.astype(jnp.bfloat16).reshape(BLOCK * rows, width)
        flat = block.reshape(BLOCK * rows, width)
        summed = flat.astype(jnp.float32) + dot(mixed.astype(jnp.bfloat16), mix_v[layer])
        summed = summed + dot(context, ctx_v[layer])
        centered = summed - jnp.mean(summed, axis=-1, keepdims=True)
        variance = jnp.mean(centered * centered, axis=-1, keepdims=True)
        normed = centered * lax.rsqrt(variance + EPS) * gains[layer : layer + 1, :]
        normed = normed.astype(jnp.bfloat16)
        hidden = jnp.maximum(dot(normed, up_v[layer]), 0.0).astype(jnp.bfloat16)
        following = normed.astype(jnp.float32) + dot(hidden, down_v[layer])
        following = masked(following.reshape(BLOCK, rows, width), step, first_pos)
        if layer + 1 < layers:
            x[layer + 1, part] = following
            add_totals(layer + 1, step, following)
            send_halos(layer + 1, step)
        else:
            result[part] = following
            out_copy(step).start()
        return carry

    def out_copy(step):
        part = pl.ds(step * BLOCK, BLOCK)
        return pltpu.make_async_copy(result.at[part], out.at[part], out_sem.at[step])

    for layer in range(layers):
        start_group(layer)
        lax.fori_loop(0, steps // 2, functools.partial(own_step, layer), 0)
        finish_group_start_cross(layer)
        lax.fori_loop(steps // 2, steps, functools.partial(own_step, layer), 0)
        if layer == 0:
            for copy in weight_copies:
                copy.wait()
        finish_cross(layer)
        lax.fori_loop(0, steps, functools.partial(layer_step, layer), 0)

    for layer in range(layers):
        wait_sum_sends(layer)
        for step in range(steps):
            wait_halo_sends(layer, step)
    for step in range(steps):
        out_copy(step).wait()


def per_device(count, events, lengths, w_mix, w_context, gains, w_up, w_down):
    users, rows, width = events.shape
    layers, _, hidden = w_up.shape
    steps = users // BLOCK
    group = group_size(count)
    groups = count // group
    per_dot = ROWS // rows
    bf16, f32 = jnp.bfloat16, jnp.float32
    vmem, dma = pltpu.VMEM, pltpu.SemaphoreType.DMA
    scratch = [
        vmem((layers, users, rows, width), bf16),
        vmem((users, rows, width), bf16),
        vmem((layers, users, HALF, width), bf16),
        vmem((layers, users, HALF, width), bf16),
        vmem((users, rows, width), f32),
        vmem(w_mix.shape, bf16),
        vmem(w_context.shape, bf16),
        vmem(w_up.shape, bf16),
        vmem(w_down.shape, bf16),
        vmem((ROWS, ROWS), f32),
        vmem((ROWS, 2 * per_dot * HALF), f32),
        vmem((ROWS, ROWS), bf16),
        vmem((rows, width), f32),
        vmem((BLOCK, BLOCK * rows), bf16),
        vmem((layers, users, width), f32),
        vmem((layers, group - 1, users, width), f32),
        vmem((layers, users, width), f32),
        vmem((layers, groups - 1, users, width), f32),
        vmem((layers, users, width), f32),
        dma((steps,)),
        dma((4,)),
        dma((steps,)),
        dma((layers, 2, steps)),
        dma((layers, 2, steps)),
        dma((layers, group - 1)),
        dma((layers, group - 1)),
        dma((layers, groups - 1)),
        dma((layers, groups - 1)),
    ]
    anywhere = pl.BlockSpec(memory_space=pl.ANY)
    return pl.pallas_call(
        functools.partial(kernel, count),
        out_shape=jax.ShapeDtypeStruct(events.shape, bf16),
        in_specs=[
            pl.BlockSpec(memory_space=pltpu.SMEM),
            pl.BlockSpec(memory_space=pltpu.VMEM),
        ]
        + [anywhere] * 5,
        out_specs=anywhere,
        scratch_shapes=scratch,
        compiler_params=pltpu.CompilerParams(
            collective_id=0, has_side_effects=True, vmem_limit_bytes=60 * 1024 * 1024
        ),
        name="layers",
    )(lengths, gains, events, w_mix, w_context, w_up, w_down)


def solution(mesh):
    placed = (P("user", "tm", None), P("user"), P(), P(), P(), P(), P())
    return jax.shard_map(
        functools.partial(per_device, mesh.shape["tm"]),
        mesh=mesh,
        in_specs=placed,
        out_specs=P("user", "tm", None),
        check_vma=False,
    )
```
